128 devices in a mesh: wide: 32 (over x, z, core), narrow: 4 (over y).
Axes of the slice: x: 4, y: 4, z: 4, core: 2. Of those that a mesh axis runs over, the one named last changes fastest.
Arguments:
- tokens: bfloat16 [4096, 3584], P(('wide', 'narrow')), may hold values from -6 to 6
- norm_gain: float32 [3584], replicated, may hold values from 0.1 to 1.9
- expert_ids: int32 [4096, 8], P(('wide', 'narrow')), may hold values from 0 to 127, all different within a row; in each aligned block of 32 rows (0 to 31, 32 to 63, ...) at most 3 rows name the same one
- gate_values: int32 [4096, 8], P(('wide', 'narrow')), may hold values from 1 to 65535
- w_gate: bfloat16 [128, 3584, 1024], P(('wide', 'narrow')), may hold values from -0.09375 to 0.09375
- w_up: bfloat16 [128, 3584, 1024], P(('wide', 'narrow')), may hold values from -0.09375 to 0.09375
- w_down: bfloat16 [128, 1024, 3584], P(('wide', 'narrow')), may hold values from -0.1875 to 0.1875
- queries: bfloat16 [256, 73728], P(('wide', 'narrow')), may hold values from -48 to 48
- latent_cache: bfloat16 [256, 589824], P(('wide', 'narrow')), may hold values from -8 to 8
- cache_lengths: int32 [256], P(('wide', 'narrow')), may hold values from 2 to 1024, as said below
Outputs:
- combined: bfloat16 [4096, 3584], P(('wide', 'narrow'))
- attention: bfloat16 [256, 65536], P(('wide', 'narrow'))
The draws below stay inside these ranges and needn't reach their ends.
Inputs may be any that keep to these rules, and one draw needn't show every extreme that they name: `expert_ids`: each row names 8 different experts; among the 32 rows of one device no expert is named more than 3 times, and some device's rows name some expert exactly 3 times. `cache_lengths`: some request has exactly 1024 cached positions.
All inputs are finite; a program needn't handle non-finite values.
Results may differ from the reference program's by a relative error of at most 0.0068.
Values may be sent and summed in bfloat16 or wider, within the bound.
No kernel may reach another device: no remote copies, remote signals or barrier semaphores. Data moves between devices by JAX's collectives and lax.ppermute only.
A program may use at most 128 MiB of HBM per device.

```python
import math
import jax
import jax.numpy as jnp
import numpy as np
from jax import lax

D = 3584
HID = 1024
HEADS = 128
LATENT = 512
QK = 576
TOP = 8
TOK_DEV = 32
CTX = 1024
EXPERTS = 128
CAP = 3
TOKENS = 4096
REQS = 256


def cache_values(key):
    values = jax.random.normal(jax.random.fold_in(key, 11), (REQS, CTX, QK), jnp.float32)
    return jnp.clip(values, -8.0, 8.0)


def draw_latent_cache(key, part):
    return cache_values(key).reshape(REQS, CTX * QK).astype(jnp.bfloat16)


def draw_queries(key, part):
    result = jax.random.normal(jax.random.fold_in(key, 21), (REQS, HEADS, QK), jnp.float32)
    result = jnp.clip(result, -6.0, 6.0)
    return jnp.clip(result, -48.0, 48.0).reshape(REQS, HEADS * QK).astype(jnp.bfloat16)


def draw_cache_lengths(key, part):
    base_lengths = jax.random.randint(jax.random.fold_in(key, 31), (REQS,), 2, CTX + 1)
    full_one = jax.random.randint(jax.random.fold_in(key, 32), (), 0, REQS)
    return jnp.where(jnp.arange(REQS) == full_one, CTX, base_lengths).astype(jnp.int32)


def with_ends(values, own_key, smallest, largest):
    longest = values.shape.index(max(values.shape))
    spots = []
    for shift in (0, 1):
        where = [jax.random.randint(jax.random.fold_in(own_key, axis), (), 0, length) for axis, length in enumerate(values.shape)]
        where[longest] = (where[longest] + shift) % values.shape[longest]
        spots.append(tuple(where))
    return values.at[spots[0]].set(smallest).at[spots[1]].set(largest)


def block_levels(stream_key, extent, split, least, largest):
    def one(dim, blocks):
        draws = jax.random.uniform(jax.random.fold_in(jax.random.fold_in(stream_key, 6), dim), (blocks,), jnp.float32, least / len(split), largest / len(split))
        return jnp.repeat(jnp.exp(draws), extent[dim] // blocks).reshape((-1,) + (1,) * (len(extent) - dim - 1))

    level = one(*split[0])
    for cut in split[1:]:
        level = level * one(*cut)
    return level


def routed_block(key, own, number, rows, amount, top, most, lean):
    sequence = jax.random.permutation(key, amount)
    crowded, usual = shares(amount, rows * top, most, lean, True), shares(amount, rows * top, most, lean, False)
    places = jnp.arange(amount)

    def named(tallies, rotation):
        used = int((tallies > 0).sum())
        fixed = max(1, used // 4)
        passed = fixed + (places - fixed + rotation * (used - fixed)) % max(1, amount - fixed)
        return jnp.zeros((amount,), jnp.int32).at[sequence[jnp.where(places < fixed, places, passed)]].set(jnp.asarray(tallies, jnp.int32))

    tallies = jnp.where(number % 4 == 0, named(crowded, number // 4), named(usual, number - number // 4 - 1))
    mixed = jax.random.permutation(jax.random.fold_in(own, 3), amount)
    giver, receiver = mixed[0:amount // 2 * 2:2], mixed[1:amount // 2 * 2:2]
    slack = jnp.minimum(tallies[giver] - 1, most - tallies[receiver]) // 2
    slack = jnp.where((giver == sequence[0]) | (receiver == sequence[0]) | (tallies[receiver] == 0), 0, jnp.maximum(slack, 0))
    passed = jax.random.randint(jax.random.fold_in(own, 4), (amount // 2,), 0, 1 << 20) % (slack + 1)
    tallies = tallies.at[giver].add(-passed).at[receiver].add(passed)
    members = jnp.searchsorted(jnp.cumsum(tallies), jnp.arange(rows * top), side="right").astype(jnp.int32)
    table = members.reshape(top, rows).T
    table = table[jax.random.permutation(jax.random.fold_in(own, 1), rows)]
    rotation = jax.random.randint(jax.random.fold_in(own, 2), (rows, 1), 0, top)
    return jnp.take_along_axis(table, (jnp.arange(top)[None, :] + rotation) % top, axis=1)


def shares(number_of, total, reach, lean, full):
    loads = [(1 << 20) // math.isqrt(grade ** lean) + 1 for grade in range(1, number_of + 1)]
    largest = reach if full else min(reach, max(-(-total // number_of), total * loads[0] // sum(loads)))
    least = 1 if total - largest >= number_of - 1 else 0
    given, spare = [largest] + [least] * (number_of - 1), total - largest - least * (number_of - 1)
    while spare > 0:
        free = [i for i in range(1, number_of) if given[i] < largest] or [i for i in range(1, number_of) if given[i] < reach]
        pool, left = sum([loads[i] for i in free]), spare
        for i in free:
            addition = min(reach - given[i], max(1, left * loads[i] // pool), spare)
            given[i] = given[i] + addition
            spare = spare - addition
    return np.array(given)


def scatter_about(rng, shape, spread, limit, pieces=(), kind=jnp.bfloat16):
    level = block_levels(rng, shape, pieces, -0.22, 0.18) if pieces else 1.0
    entries = jax.random.normal(rng, shape, jnp.float32) * spread * level
    return jnp.minimum(jnp.maximum(entries, -limit), limit).astype(kind)


def setup_inputs(seed: int = 0) -> dict:
    arg_keys = jax.random.split(jax.random.key(seed), 11)
    tokens = scatter_about(arg_keys[0], (TOKENS, D), 1.0, 6.0, ((0, 128),))
    norm_gain = jnp.clip(1.0 + 0.18 * jax.random.normal(arg_keys[1], (D,), jnp.float32), 0.1, 1.9)
    expert_ids_keys = jax.random.split(jax.random.fold_in(arg_keys[2], 1), TOKENS // TOK_DEV)
    expert_ids_turns = jax.random.permutation(jax.random.fold_in(arg_keys[2], 3), TOKENS // TOK_DEV)
    expert_ids = jax.vmap(lambda own, number: routed_block(jax.random.fold_in(arg_keys[2], 2), own, number, TOK_DEV, EXPERTS, TOP, CAP, 2))(expert_ids_keys, expert_ids_turns).reshape((TOKENS, TOP))
    gate_values = with_ends(jax.random.randint(arg_keys[3], (TOKENS, TOP), 1, 65536), jax.random.fold_in(arg_keys[3], 1), 1, 65535).astype(jnp.int32)
    w_gate = scatter_about(arg_keys[4], (EXPERTS, D, HID), D ** -0.5, 0.09375, ((0, 128),))
    w_up = scatter_about(arg_keys[5], (EXPERTS, D, HID), D ** -0.5, 0.09375, ((0, 128),))
    w_down = scatter_about(arg_keys[6], (EXPERTS, HID, D), HID ** -0.5, 0.1875, ((0, 128),))
    queries = draw_queries(jax.random.fold_in(arg_keys[10], 71), 0)
    latent_cache = draw_latent_cache(jax.random.fold_in(arg_keys[10], 71), 0)
    cache_lengths = draw_cache_lengths(jax.random.fold_in(arg_keys[10], 71), 0)
    return dict(tokens=tokens, norm_gain=norm_gain, expert_ids=expert_ids, gate_values=gate_values, w_gate=w_gate, w_up=w_up, w_down=w_down, queries=queries, latent_cache=latent_cache, cache_lengths=cache_lengths)


score_scale = 192.0 ** (-0.5)
norm_eps = 1e-06
gate_unit = 32768.0

def attend_one(inputs):
    query_rows, cache_rows, length_one = inputs
    query_block = query_rows.reshape(HEADS, QK)
    cache_block = cache_rows.reshape(CTX, QK)
    scores = jnp.dot(query_block, cache_block.T, preferred_element_type=jnp.float32) * score_scale
    visible = jnp.arange(CTX, dtype=jnp.int32)[None, :] < length_one
    scores = jnp.where(visible, scores, -jnp.inf)
    peak = lax.optimization_barrier(jnp.max(scores, axis=1, keepdims=True))
    weights = jnp.exp(scores - peak)
    weights = (weights / lax.optimization_barrier(jnp.sum(weights, axis=1, keepdims=True))).astype(jnp.bfloat16)
    mixed = jnp.dot(weights, cache_block[:, :LATENT], preferred_element_type=jnp.float32)
    return mixed.astype(jnp.bfloat16).reshape(HEADS * LATENT)

def reference(tokens, norm_gain, expert_ids, gate_values, w_gate, w_up, w_down, queries, latent_cache, cache_lengths):
    attention = lax.map(attend_one, (queries, latent_cache, cache_lengths))
    token_float = tokens.astype(jnp.float32)
    squares = lax.optimization_barrier(jnp.mean(token_float * token_float, axis=1, keepdims=True))
    normed = (token_float * lax.rsqrt(squares + norm_eps) * norm_gain).astype(jnp.bfloat16)
    flat_ids = expert_ids.reshape(-1).astype(jnp.int32)
    pairs_count = TOKENS * TOP
    order = jnp.argsort(flat_ids, stable=True).astype(jnp.int32)
    expert_range = jnp.arange(EXPERTS, dtype=jnp.int32)
    counts = lax.optimization_barrier(jnp.sum((flat_ids[:, None] == expert_range[None, :]).astype(jnp.int32), axis=0))
    starts = jnp.cumsum(counts) - counts
    most_rows = EXPERTS * CAP

    def one_expert(inputs):
        expert, gate_matrix, up_matrix, down_matrix = inputs
        offsets = jnp.arange(most_rows, dtype=jnp.int32)
        usable = offsets < counts[expert]
        picks = order[jnp.minimum(starts[expert] + offsets, pairs_count - 1)]
        rows_in = jnp.where(usable[:, None], normed[picks // TOP], jnp.zeros((), jnp.bfloat16))
        gate_part = jnp.dot(rows_in, gate_matrix, preferred_element_type=jnp.float32)
        up_part = jnp.dot(rows_in, up_matrix, preferred_element_type=jnp.float32)
        inner = (jax.nn.silu(gate_part) * up_part).astype(jnp.bfloat16)
        outputs = jnp.dot(inner, down_matrix, preferred_element_type=jnp.float32).astype(jnp.bfloat16)
        places = jnp.where(usable, picks, pairs_count).astype(jnp.int32)
        return (places, outputs)
    places, outputs = lax.map(one_expert, (expert_range, w_gate, w_up, w_down))
    pair_out = jnp.zeros((pairs_count + 1, D), jnp.bfloat16)
    pair_out = pair_out.at[places.reshape(-1)].set(outputs.reshape(-1, D))[:pairs_count]
    gate_weights = gate_values.astype(jnp.float32) / gate_unit
    expert_sum = lax.optimization_barrier(jnp.sum(gate_weights[:, :, None] * pair_out.reshape(TOKENS, TOP, D).astype(jnp.float32), axis=1))
    combined = (token_float + expert_sum).astype(jnp.bfloat16)
    return (combined, attention)
```

```python
import jax
import jax.numpy as jnp
from jax import lax
from jax.experimental import pallas as pl
from jax.experimental.pallas import tpu as pltpu
from jax.sharding import PartitionSpec as P

HEADS = 128
LATENT = 512
QK = 576
TOP = 8
CTX = 1024
WIDTH = 3584
HID = 1024
EXPERTS = 128
TOK = 32
ROWS = 8
LANES = 1408
TAIL = 768
SENT = EXPERTS * ROWS

score_scale = 192.0 ** (-0.5)
norm_eps = 1e-06
gate_unit = 32768.0
f32 = jnp.float32
bf16 = jnp.bfloat16


def iota(shape, dim):
    return lax.broadcasted_iota(jnp.int32, shape, dim)


def ones_where(mask):
    return jnp.where(mask, 1.0, 0.0).astype(bf16)


def dot(a, b):
    return jnp.dot(a, b, preferred_element_type=f32)


def dispatch_kernel(tokens, gain, ids, send, stacked):
    rows = tokens[...].astype(f32)
    squares = jnp.mean(rows * rows, axis=1, keepdims=True)
    normed = (rows * lax.rsqrt(squares + norm_eps) * gain[...]).astype(bf16)
    last = 2 * LANES
    stacked[0:32, :] = normed[:, 0:LANES]
    stacked[32:64, :] = normed[:, LANES:last]
    stacked[64:96, 0:TAIL] = normed[:, last:]
    stacked[64:96, TAIL:] = normed[:, last : last + 640]
    stacked[96:128, 0:TAIL] = normed[:, last:]
    stacked[96:128, TAIL:896] = normed[:, last + 640 :]
    stacked[96:128, 896:] = jnp.zeros((32, LANES - 896), bf16)
    expert = iota((EXPERTS, TOK), 0)
    member = jnp.zeros((EXPERTS, TOK), f32)
    for k in range(TOP):
        member = member + jnp.where(expert == ids[k : k + 1, :], 1.0, 0.0)
    earlier = ones_where(iota((TOK, TOK), 0) < iota((TOK, TOK), 1))
    code = member * (dot(member.astype(bf16), earlier) + 1.0)
    repeat = ones_where((iota((TOK, 128), 1) & 31) == iota((TOK, 128), 0))
    code = dot(code.astype(bf16), repeat).astype(bf16)
    spread = ones_where((iota((SENT, 128), 0) >> 3) == iota((SENT, 128), 1))
    code = dot(spread, code).astype(jnp.int32)
    row = iota((SENT, 128), 0) & 7
    source = jnp.where(row < 6, row & 1, row - 4)
    mine = source == (iota((SENT, 128), 1) >> 5)
    front = jnp.where(row < 6, row >> 1, row - 6) + 1
    back = jnp.where(row < 6, row >> 1, 2) + 1
    pick_front = ones_where(mine & (code == front))
    pick_back = ones_where(mine & (code == back))
    send[:, 0:TAIL] = dot(pick_front, stacked[:, 0:TAIL]).astype(bf16)
    send[:, TAIL:] = dot(pick_back, stacked[:, TAIL:]).astype(bf16)


def expert_kernel(
    recv, gate_hbm, up_hbm, down_hbm, send, gate, up, down, rows_in, inner, mixed, sems
):
    steps = HID // 256
    parts = ((0, LANES), (LANES, LANES), (2 * LANES, TAIL))

    def fetch(step):
        cols = pl.ds(step * 256, 256)
        return (
            pltpu.make_async_copy(gate_hbm.at[0, :, cols], gate.at[step], sems.at[0, step]),
            pltpu.make_async_copy(up_hbm.at[0, :, cols], up.at[step], sems.at[1, step]),
        )

    def fetch_down(step):
        rows = pl.ds(step * 256, 256)
        return pltpu.make_async_copy(
            down_hbm.at[0, rows, :], down.at[rows, :], sems.at[2, step]
        )

    for step in range(steps):
        for copy in fetch(step):
            copy.start()
    for step in range(steps):
        fetch_down(step).start()
    line = iota((256, 256), 0)
    column = iota((256, 256), 1)
    gather = ones_where(column == 8 * (line & 31) + (line >> 5))
    scatter = ones_where(line == 8 * (column & 31) + (column >> 5))
    for group in range(4):
        block = dot(gather, recv[group * 256 : (group + 1) * 256, :]).astype(bf16)
        for slot in range(3):
            at = pl.ds(group * 96 + slot * 32, 32)
            rows_in[at, 0:LANES] = block[64 * slot : 64 * slot + 32, :]
            rows_in[at, LANES : 2 * LANES] = block[64 * slot + 32 : 64 * slot + 64, :]
            if slot < 2:
                rows_in[at, 2 * LANES :] = block[192 + 32 * slot : 224 + 32 * slot, 0:TAIL]
            else:
                rows_in[at, 2 * LANES : 2 * LANES + 640] = block[192:224, TAIL:]
                rows_in[at, 2 * LANES + 640 :] = block[224:256, TAIL:896]

    @pl.loop(0, steps)
    def _(step):
        for copy in fetch(step):
            copy.wait()
        gate_part = dot(rows_in[...], gate[step])
        up_part = dot(rows_in[...], up[step])
        value = gate_part / (1.0 + jnp.exp(-gate_part)) * up_part
        inner[:, pl.ds(pl.multiple_of(step * 256, 256), 256)] = value.astype(bf16)

    for step in range(steps):
        fetch_down(step).wait()
    for group in range(4):
        mixed[group, 224:256, 896:] = jnp.zeros((32, LANES - 896), bf16)
    for part, (start, width) in enumerate(parts):
        result = dot(inner[...], down[:, start : start + width]).astype(bf16)
        for group in range(4):
            for slot in range(3):
                piece = result[group * 96 + slot * 32 : group * 96 + slot * 32 + 32, :]
                if part < 2:
                    at = 64 * slot + 32 * part
                    mixed[group, at : at + 32, :] = piece
                elif slot < 2:
                    mixed[group, 192 + 32 * slot : 224 + 32 * slot, 0:TAIL] = piece
                else:
                    mixed[group, 192:224, TAIL:] = piece[:, 0:640]
                    mixed[group, 224:256, TAIL:896] = piece[:, 640:]
    for group in range(4):
        send[group * 256 : (group + 1) * 256, :] = dot(scatter, mixed[group]).astype(bf16)


def weights_kernel(ids, gates, front, tail_a, tail_b):
    expert = iota((TOK, EXPERTS), 1)
    member = jnp.zeros((TOK, EXPERTS), f32)
    high = jnp.zeros((TOK, EXPERTS), f32)
    low = jnp.zeros((TOK, EXPERTS), f32)
    for k in range(TOP):
        hit = expert == ids[:, k : k + 1]
        value = gates[:, k : k + 1]
        member = member + jnp.where(hit, 1.0, 0.0)
        high = high + jnp.where(hit, (value >> 8).astype(f32), 0.0)
        low = low + jnp.where(hit, (value & 255).astype(f32), 0.0)
    earlier = ones_where(iota((TOK, TOK), 1) < iota((TOK, TOK), 0))
    code = (member * (dot(earlier, member.astype(bf16)) + 1.0)).astype(bf16)
    high = high.astype(bf16)
    low = low.astype(bf16)
    code = jnp.concatenate([code] * 4, axis=0)
    value = jnp.concatenate([high, low, high, low], axis=0)
    spread = ones_where((iota((EXPERTS, SENT), 1) >> 3) == iota((EXPERTS, SENT), 0))
    code = dot(code, spread).astype(jnp.int32)
    value = dot(value, spread)
    row = iota((128, SENT), 1) & 7
    pair = iota((128, SENT), 0) >> 6
    keep = (row < 6) & ((row & 1) == pair) & (code == (row >> 1) + 1)
    front[...] = jnp.where(keep, value, 0.0).astype(bf16)
    keep = (row >= 6) & (pair == 0) & (code == row - 5)
    tail_a[...] = jnp.where(keep, value, 0.0).astype(bf16)
    keep = (row == pair + 6) & (code == 3)
    tail_b[...] = jnp.where(keep, value, 0.0).astype(bf16)


def combine_kernel(recv, tokens, front, tail_a, tail_b, combined):
    def join(sums, start):
        return (sums[start : start + 32] * 256.0 + sums[start + 32 : start + 64]) * (
            1.0 / gate_unit
        )

    sums = dot(front[...], recv[...])
    end = 2 * LANES
    combined[:, 0:LANES] = (tokens[:, 0:LANES].astype(f32) + join(sums, 0)).astype(bf16)
    combined[:, LANES:end] = (tokens[:, LANES:end].astype(f32) + join(sums, 64)).astype(bf16)
    first = join(dot(tail_a[...], recv[:, 0:TAIL]), 0)
    second = dot(tail_b[...], recv[:, TAIL:])
    rest = tokens[:, end:].astype(f32)
    combined[:, end : end + 640] = (rest[:, 0:640] + first[:, 0:640] + join(second, 0)).astype(
        bf16
    )
    combined[:, end + 640 :] = (
        rest[:, 640:] + first[:, 640:] + join(second[:, 0:128], 64)
    ).astype(bf16)


def call(kernel, outs, scratch=(), in_specs=None, flops=0, moved=0, limit=None, name=None):
    def whole(_):
        return pl.BlockSpec(memory_space=pltpu.VMEM)

    single = not isinstance(outs, (list, tuple))

    def run(*args):
        return pl.pallas_call(
            kernel,
            out_shape=outs,
            in_specs=in_specs or [whole(a) for a in args],
            out_specs=whole(outs) if single else [whole(o) for o in outs],
            scratch_shapes=list(scratch),
            cost_estimate=pl.CostEstimate(flops=flops, bytes_accessed=moved, transcendentals=0),
            compiler_params=pltpu.CompilerParams(vmem_limit_bytes=limit),
            name=name,
        )(*args)

    return run


def attend_local(queries, latent_cache, cache_lengths):
    requests = queries.shape[0]
    query_block = queries.reshape(requests, HEADS, QK)
    cache_block = latent_cache.reshape(requests, CTX, QK)
    scores = (
        jnp.einsum("rhq,rtq->rht", query_block, cache_block, preferred_element_type=jnp.float32)
        * score_scale
    )
    visible = jnp.arange(CTX, dtype=jnp.int32)[None, None, :] < cache_lengths[:, None, None]
    scores = jnp.where(visible, scores, -jnp.inf)
    peak = jnp.max(scores, axis=2, keepdims=True)
    weights = jnp.exp(scores - peak)
    weights = (weights / jnp.sum(weights, axis=2, keepdims=True)).astype(jnp.bfloat16)
    mixed = jnp.einsum(
        "rht,rtl->rhl", weights, cache_block[:, :, :LATENT], preferred_element_type=jnp.float32
    )
    return mixed.astype(jnp.bfloat16).reshape(requests, HEADS * LATENT)


def exchange(rows):
    blocks = rows.reshape(EXPERTS, ROWS, LANES)
    blocks = lax.all_to_all(blocks, ("wide", "narrow"), split_axis=0, concat_axis=0, tiled=True)
    return blocks.reshape(SENT, LANES)


def on_device(
    tokens,
    norm_gain,
    expert_ids,
    gate_values,
    w_gate,
    w_up,
    w_down,
    queries,
    latent_cache,
    cache_lengths,
):
    sent_shape = jax.ShapeDtypeStruct((SENT, LANES), bf16)
    send = call(
        dispatch_kernel,
        sent_shape,
        scratch=[pltpu.VMEM((128, LANES), bf16)],
        flops=2 * SENT * 128 * LANES,
        moved=4 * 1024 * 1024,
        limit=32 * 1024 * 1024,
        name="dispatch",
    )(tokens, norm_gain.reshape(1, WIDTH), expert_ids.T)
    recv = exchange(send)
    anywhere = pl.BlockSpec(memory_space=pl.ANY)
    worked = call(
        expert_kernel,
        sent_shape,
        scratch=[
            pltpu.VMEM((4, WIDTH, 256), bf16),
            pltpu.VMEM((4, WIDTH, 256), bf16),
            pltpu.VMEM((HID, WIDTH), bf16),
            pltpu.VMEM((384, WIDTH), bf16),
            pltpu.VMEM((384, HID), bf16),
            pltpu.VMEM((4, 256, LANES), bf16),
            pltpu.SemaphoreType.DMA((3, 4)),
        ],
        in_specs=[pl.BlockSpec(memory_space=pltpu.VMEM), anywhere, anywhere, anywhere],
        flops=6 * 384 * WIDTH * HID,
        moved=28 * 1024 * 1024,
        limit=60 * 1024 * 1024,
        name="experts",
    )(recv, w_gate, w_up, w_down)
    returned = exchange(worked)
    weight_shape = jax.ShapeDtypeStruct((128, SENT), bf16)
    weights = call(
        weights_kernel,
        [weight_shape] * 3,
        flops=4 * 128 * 128 * SENT,
        moved=1024 * 1024,
        limit=32 * 1024 * 1024,
        name="weights",
    )(expert_ids, gate_values)
    combined = call(
        combine_kernel,
        jax.ShapeDtypeStruct((TOK, WIDTH), bf16),
        flops=4 * 128 * SENT * LANES,
        moved=4 * 1024 * 1024,
        limit=32 * 1024 * 1024,
        name="combine",
    )(returned, tokens, *weights)
    attention = attend_local(queries, latent_cache, cache_lengths)
    return (combined, attention)


def solution(mesh):
    both = ("wide", "narrow")
    in_specs = (
        P(both, None),
        P(),
        P(both, None),
        P(both, None),
        P(both, None, None),
        P(both, None, None),
        P(both, None, None),
        P(both, None),
        P(both, None),
        P(both),
    )
    out_specs = (P(both, None), P(both, None))
    return jax.shard_map(
        on_device, mesh=mesh, in_specs=in_specs, out_specs=out_specs, check_vma=False
    )
```

```python
import jax
import jax.numpy as jnp
from jax import lax
from jax.experimental import pallas as pl
from jax.experimental.pallas import tpu as pltpu
from jax.sharding import PartitionSpec as P

HEADS = 128
LATENT = 512
QK = 576
TOP = 8
CTX = 1024
WIDTH = 3584
HID = 1024
EXPERTS = 128
TOK = 32
ROWS = 8
LANES = 1408
TAIL = 768
SENT = EXPERTS * ROWS

score_scale = 192.0 ** (-0.5)
norm_eps = 1e-06
gate_unit = 32768.0
f32 = jnp.float32
bf16 = jnp.bfloat16


def iota(shape, dim):
    return lax.broadcasted_iota(jnp.int32, shape, dim)


def ones_where(mask):
    return jnp.where(mask, 1.0, 0.0).astype(bf16)


def dot(a, b):
    return jnp.dot(a, b, preferred_element_type=f32)


def dispatch_kernel(tokens, gain, ids, send, stacked):
    rows = tokens[...].astype(f32)
    squares = jnp.mean(rows * rows, axis=1, keepdims=True)
    normed = (rows * lax.rsqrt(squares + norm_eps) * gain[...]).astype(bf16)
    last = 2 * LANES
    stacked[0:32, :] = normed[:, 0:LANES]
    stacked[32:64, :] = normed[:, LANES:last]
    stacked[64:96, 0:TAIL] = normed[:, last:]
    stacked[64:96, TAIL:] = normed[:, last : last + 640]
    stacked[96:128, 0:TAIL] = normed[:, last:]
    stacked[96:128, TAIL:896] = normed[:, last + 640 :]
    stacked[96:128, 896:] = jnp.zeros((32, LANES - 896), bf16)
    expert = iota((EXPERTS, TOK), 0)
    member = jnp.zeros((EXPERTS, TOK), f32)
    for k in range(TOP):
        member = member + jnp.where(expert == ids[k : k + 1, :], 1.0, 0.0)
    earlier = ones_where(iota((TOK, TOK), 0) < iota((TOK, TOK), 1))
    code = member * (dot(member.astype(bf16), earlier) + 1.0)
    repeat = ones_where((iota((TOK, 128), 1) & 31) == iota((TOK, 128), 0))
    code = dot(code.astype(bf16), repeat).astype(bf16)
    spread = ones_where((iota((SENT, 128), 0) >> 3) == iota((SENT, 128), 1))
    code = dot(spread, code).astype(jnp.int32)
    row = iota((SENT, 128), 0) & 7
    source = jnp.where(row < 6, row & 1, row - 4)
    mine = source == (iota((SENT, 128), 1) >> 5)
    front = jnp.where(row < 6, row >> 1, row - 6) + 1
    back = jnp.where(row < 6, row >> 1, 2) + 1
    pick_front = ones_where(mine & (code == front))
    pick_back = ones_where(mine & (code == back))
    send[:, 0:TAIL] = dot(pick_front, stacked[:, 0:TAIL]).astype(bf16)
    send[:, TAIL:] = dot(pick_back, stacked[:, TAIL:]).astype(bf16)


def expert_kernel(
    recv, gate, up_hbm, down_hbm, send, up, down, rows_in, inner, mixed, packed, sems
):
    steps = HID // 256
    parts = ((0, LANES), (LANES, LANES), (2 * LANES, TAIL))

    def fetch(step):
        cols = pl.ds(step * 256, 256)
        return pltpu.make_async_copy(up_hbm.at[0, :, cols], up.at[step], sems.at[0, step])

    def fetch_down(step):
        rows = pl.ds(step * 256, 256)
        return pltpu.make_async_copy(
            down_hbm.at[0, rows, :], down.at[rows, :], sems.at[1, step]
        )

    def store(group):
        return pltpu.make_async_copy(
            packed.at[group], send.at[pl.ds(group * 256, 256), :], sems.at[2, group]
        )

    for step in range(steps):
        fetch(step).start()
    for step in range(steps):
        fetch_down(step).start()
    line = iota((256, 256), 0)
    column = iota((256, 256), 1)
    gather = ones_where(column == 8 * (line & 31) + (line >> 5))
    scatter = ones_where(line == 8 * (column & 31) + (column >> 5))
    for group in range(4):
        block = dot(gather, recv[group * 256 : (group + 1) * 256, :]).astype(bf16)
        for slot in range(3):
            at = pl.ds(group * 96 + slot * 32, 32)
            rows_in[at, 0:LANES] = block[64 * slot : 64 * slot + 32, :]
            rows_in[at, LANES : 2 * LANES] = block[64 * slot + 32 : 64 * slot + 64, :]
            if slot < 2:
                rows_in[at, 2 * LANES :] = block[192 + 32 * slot : 224 + 32 * slot, 0:TAIL]
            else:
                rows_in[at, 2 * LANES : 2 * LANES + 640] = block[192:224, TAIL:]
                rows_in[at, 2 * LANES + 640 :] = block[224:256, TAIL:896]

    @pl.loop(0, steps)
    def _(step):
        cols = pl.ds(pl.multiple_of(step * 256, 256), 256)
        gate_part = dot(rows_in[...], gate[0, :, cols])
        fetch(step).wait()
        up_part = dot(rows_in[...], up[step])
        value = gate_part / (1.0 + jnp.exp(-gate_part)) * up_part
        inner[:, cols] = value.astype(bf16)

    for step in range(steps):
        fetch_down(step).wait()
    for group in range(4):
        mixed[group, 224:256, 896:] = jnp.zeros((32, LANES - 896), bf16)
    for part, (start, width) in enumerate(parts):
        result = dot(inner[...], down[:, start : start + width]).astype(bf16)
        for group in range(4):
            for slot in range(3):
                piece = result[group * 96 + slot * 32 : group * 96 + slot * 32 + 32, :]
                if part < 2:
                    at = 64 * slot + 32 * part
                    mixed[group, at : at + 32, :] = piece
                elif slot < 2:
                    mixed[group, 192 + 32 * slot : 224 + 32 * slot, 0:TAIL] = piece
                else:
                    mixed[group, 192:224, TAIL:] = piece[:, 0:640]
                    mixed[group, 224:256, TAIL:896] = piece[:, 640:]
    for group in range(4):
        packed[group] = dot(scatter, mixed[group]).astype(bf16)
        store(group).start()
    for group in range(4):
        store(group).wait()


def weights_kernel(ids, gates, picks):
    expert = iota((TOK, EXPERTS), 1)
    member = jnp.zeros((TOK, EXPERTS), f32)
    high = jnp.zeros((TOK, EXPERTS), f32)
    low = jnp.zeros((TOK, EXPERTS), f32)
    for k in range(TOP):
        hit = expert == ids[:, k : k + 1]
        value = gates[:, k : k + 1]
        member = member + jnp.where(hit, 1.0, 0.0)
        high = high + jnp.where(hit, (value >> 8).astype(f32), 0.0)
        low = low + jnp.where(hit, (value & 255).astype(f32), 0.0)
    earlier = ones_where(iota((TOK, TOK), 1) < iota((TOK, TOK), 0))
    code = (member * (dot(earlier, member.astype(bf16)) + 1.0)).astype(bf16)
    high = high.astype(bf16)
    low = low.astype(bf16)
    code = jnp.concatenate([code] * 4, axis=0)
    value = jnp.concatenate([high, low, high, low], axis=0)
    spread = ones_where((iota((EXPERTS, SENT), 1) >> 3) == iota((EXPERTS, SENT), 0))
    code = dot(code, spread).astype(jnp.int32)
    value = dot(value, spread)
    row = iota((128, SENT), 1) & 7
    pair = iota((128, SENT), 0) >> 6
    keep = (row < 6) & ((row & 1) == pair) & (code == (row >> 1) + 1)
    picks[0:128, :] = jnp.where(keep, value, 0.0).astype(bf16)
    keep = (row >= 6) & (pair == 0) & (code == row - 5)
    picks[128:256, :] = jnp.where(keep, value, 0.0).astype(bf16)
    keep = (row == pair + 6) & (code == 3)
    picks[256:384, :] = jnp.where(keep, value, 0.0).astype(bf16)


def combine_kernel(recv, tokens, picks, combined):
    def join(sums, start):
        return (sums[start : start + 32] * 256.0 + sums[start + 32 : start + 64]) * (
            1.0 / gate_unit
        )

    sums = dot(picks[0:128, :], recv[...])
    end = 2 * LANES
    combined[:, 0:LANES] = (tokens[:, 0:LANES].astype(f32) + join(sums, 0)).astype(bf16)
    combined[:, LANES:end] = (tokens[:, LANES:end].astype(f32) + join(sums, 64)).astype(bf16)
    first = join(dot(picks[128:256, :], recv[:, 0:TAIL]), 0)
    second = dot(picks[256:384, :], recv[:, TAIL:])
    rest = tokens[:, end:].astype(f32)
    combined[:, end : end + 640] = (rest[:, 0:640] + first[:, 0:640] + join(second, 0)).astype(
        bf16
    )
    combined[:, end + 640 :] = (
        rest[:, 640:] + first[:, 640:] + join(second[:, 0:128], 64)
    ).astype(bf16)


def call(kernel, outs, scratch=(), in_specs=None, out_specs=None, flops=0, moved=0, limit=None, name=None):
    def whole(_):
        return pl.BlockSpec(memory_space=pltpu.VMEM)

    single = not isinstance(outs, (list, tuple))

    def run(*args):
        return pl.pallas_call(
            kernel,
            out_shape=outs,
            in_specs=in_specs or [whole(a) for a in args],
            out_specs=out_specs or (whole(outs) if single else [whole(o) for o in outs]),
            scratch_shapes=list(scratch),
            cost_estimate=pl.CostEstimate(flops=flops, bytes_accessed=moved, transcendentals=0),
            compiler_params=pltpu.CompilerParams(vmem_limit_bytes=limit),
            name=name,
        )(*args)

    return run


def attend_local(queries, latent_cache, cache_lengths):
    requests = queries.shape[0]
    query_block = queries.reshape(requests, HEADS, QK)
    cache_block = latent_cache.reshape(requests, CTX, QK)
    scores = (
        jnp.einsum("rhq,rtq->rht", query_block, cache_block, preferred_element_type=jnp.float32)
        * score_scale
    )
    visible = jnp.arange(CTX, dtype=jnp.int32)[None, None, :] < cache_lengths[:, None, None]
    scores = jnp.where(visible, scores, -jnp.inf)
    peak = jnp.max(scores, axis=2, keepdims=True)
    weights = jnp.exp(scores - peak)
    weights = (weights / jnp.sum(weights, axis=2, keepdims=True)).astype(jnp.bfloat16)
    mixed = jnp.einsum(
        "rht,rtl->rhl", weights, cache_block[:, :, :LATENT], preferred_element_type=jnp.float32
    )
    return mixed.astype(jnp.bfloat16).reshape(requests, HEADS * LATENT)


def exchange(rows):
    blocks = rows.reshape(EXPERTS, ROWS, LANES)
    blocks = lax.all_to_all(blocks, ("wide", "narrow"), split_axis=0, concat_axis=0, tiled=True)
    return blocks.reshape(SENT, LANES)


def on_device(
    tokens,
    norm_gain,
    expert_ids,
    gate_values,
    w_gate,
    w_up,
    w_down,
    queries,
    latent_cache,
    cache_lengths,
):
    sent_shape = jax.ShapeDtypeStruct((SENT, LANES), bf16)
    send = call(
        dispatch_kernel,
        sent_shape,
        scratch=[pltpu.VMEM((128, LANES), bf16)],
        flops=2 * SENT * 128 * LANES,
        moved=4 * 1024 * 1024,
        limit=32 * 1024 * 1024,
        name="dispatch",
    )(tokens, norm_gain.reshape(1, WIDTH), expert_ids.T)
    recv = exchange(send)
    in_hbm = pl.BlockSpec(memory_space=pltpu.HBM)
    in_vmem = pl.BlockSpec(memory_space=pltpu.VMEM)
    worked = call(
        expert_kernel,
        pltpu.HBM((SENT, LANES), bf16),
        scratch=[
            pltpu.VMEM((4, WIDTH, 256), bf16),
            pltpu.VMEM((HID, WIDTH), bf16),
            pltpu.VMEM((384, WIDTH), bf16),
            pltpu.VMEM((384, HID), bf16),
            pltpu.VMEM((4, 256, LANES), bf16),
            pltpu.VMEM((4, 256, LANES), bf16),
            pltpu.SemaphoreType.DMA((3, 4)),
        ],
        in_specs=[in_vmem, in_vmem, in_hbm, in_hbm],
        out_specs=in_hbm,
        flops=6 * 384 * WIDTH * HID,
        moved=28 * 1024 * 1024,
        limit=42 * 1024 * 1024,
        name="experts",
    )(
        recv,
        pltpu.with_memory_space_constraint(w_gate, pltpu.VMEM),
        pltpu.with_memory_space_constraint(w_up, pltpu.HBM),
        pltpu.with_memory_space_constraint(w_down, pltpu.HBM),
    )
    returned = exchange(worked)
    picks_shape = jax.ShapeDtypeStruct((384, SENT), bf16)
    weights = call(
        weights_kernel,
        picks_shape,
        flops=4 * 128 * 128 * SENT,
        moved=1024 * 1024,
        limit=32 * 1024 * 1024,
        name="weights",
    )(expert_ids, gate_values)
    combined = call(
        combine_kernel,
        jax.ShapeDtypeStruct((TOK, WIDTH), bf16),
        flops=4 * 128 * SENT * LANES,
        moved=4 * 1024 * 1024,
        limit=32 * 1024 * 1024,
        name="combine",
    )(returned, tokens, weights)
    attention = attend_local(queries, latent_cache, cache_lengths)
    return (combined, attention)


def solution(mesh):
    both = ("wide", "narrow")
    in_specs = (
        P(both, None),
        P(),
        P(both, None),
        P(both, None),
        P(both, None, None),
        P(both, None, None),
        P(both, None, None),
        P(both, None),
        P(both, None),
        P(both),
    )
    out_specs = (P(both, None), P(both, None))
    return jax.shard_map(
        on_device, mesh=mesh, in_specs=in_specs, out_specs=out_specs, check_vma=False
    )
```

```python
import jax
import jax.numpy as jnp
from jax import lax
from jax.experimental import pallas as pl
from jax.experimental.pallas import tpu as pltpu
from jax.sharding import PartitionSpec as P

HEADS = 128
LATENT = 512
QK = 576
TOP = 8
CTX = 1024
WIDTH = 3584
HID = 1024
EXPERTS = 128
TOK = 32
ROWS = 8
LANES = 1408
TAIL = 768
SENT = EXPERTS * ROWS

score_scale = 192.0 ** (-0.5)
norm_eps = 1e-06
gate_unit = 32768.0
f32 = jnp.float32
bf16 = jnp.bfloat16


def iota(shape, dim):
    return lax.broadcasted_iota(jnp.int32, shape, dim)


def ones_where(mask):
    return jnp.where(mask, 1.0, 0.0).astype(bf16)


def dot(a, b):
    return jnp.dot(a, b, preferred_element_type=f32)


def dispatch_kernel(tokens, gain, ids, send, stacked):
    rows = tokens[...].astype(f32)
    squares = jnp.mean(rows * rows, axis=1, keepdims=True)
    normed = (rows * lax.rsqrt(squares + norm_eps) * gain[...]).astype(bf16)
    last = 2 * LANES
    stacked[0:32, :] = normed[:, 0:LANES]
    stacked[32:64, :] = normed[:, LANES:last]
    stacked[64:96, 0:TAIL] = normed[:, last:]
    stacked[64:96, TAIL:] = normed[:, last : last + 640]
    stacked[96:128, 0:TAIL] = normed[:, last:]
    stacked[96:128, TAIL:896] = normed[:, last + 640 :]
    stacked[96:128, 896:] = jnp.zeros((32, LANES - 896), bf16)
    expert = iota((EXPERTS, TOK), 0)
    member = jnp.zeros((EXPERTS, TOK), f32)
    for k in range(TOP):
        member = member + jnp.where(expert == ids[k : k + 1, :], 1.0, 0.0)
    earlier = ones_where(iota((TOK, TOK), 0) < iota((TOK, TOK), 1))
    code = member * (dot(member.astype(bf16), earlier) + 1.0)
    repeat = ones_where((iota((TOK, 128), 1) & 31) == iota((TOK, 128), 0))
    code = dot(code.astype(bf16), repeat).astype(bf16)
    spread = ones_where((iota((SENT, 128), 0) >> 3) == iota((SENT, 128), 1))
    code = dot(spread, code).astype(jnp.int32)
    row = iota((SENT, 128), 0) & 7
    source = jnp.where(row < 6, row & 1, row - 4)
    mine = source == (iota((SENT, 128), 1) >> 5)
    front = jnp.where(row < 6, row >> 1, row - 6) + 1
    back = jnp.where(row < 6, row >> 1, 2) + 1
    pick_front = ones_where(mine & (code == front))
    pick_back = ones_where(mine & (code == back))
    send[:, 0:TAIL] = dot(pick_front, stacked[:, 0:TAIL]).astype(bf16)
    send[:, TAIL:] = dot(pick_back, stacked[:, TAIL:]).astype(bf16)


def expert_kernel(
    recv, gate_hbm, up_hbm, down_hbm, send, gate, up, down, rows_in, inner, mixed, sems
):
    steps = HID // 256
    parts = ((0, LANES), (LANES, LANES), (2 * LANES, TAIL))

    def fetch(step):
        cols = pl.ds(step * 256, 256)
        return (
            pltpu.make_async_copy(gate_hbm.at[0, :, cols], gate.at[step], sems.at[0, step]),
            pltpu.make_async_copy(up_hbm.at[0, :, cols], up.at[step], sems.at[1, step]),
        )

    def fetch_down(step):
        rows = pl.ds(step * 256, 256)
        return pltpu.make_async_copy(
            down_hbm.at[0, rows, :], down.at[rows, :], sems.at[2, step]
        )

    for step in range(steps):
        for copy in fetch(step):
            copy.start()
    for step in range(steps):
        fetch_down(step).start()
    line = iota((256, 256), 0)
    column = iota((256, 256), 1)
    gather = ones_where(column == 8 * (line & 31) + (line >> 5))
    scatter = ones_where(line == 8 * (column & 31) + (column >> 5))
    for group in range(4):
        block = dot(gather, recv[group * 256 : (group + 1) * 256, :]).astype(bf16)
        for slot in range(3):
            at = pl.ds(group * 96 + slot * 32, 32)
            rows_in[at, 0:LANES] = block[64 * slot : 64 * slot + 32, :]
            rows_in[at, LANES : 2 * LANES] = block[64 * slot + 32 : 64 * slot + 64, :]
            if slot < 2:
                rows_in[at, 2 * LANES :] = block[192 + 32 * slot : 224 + 32 * slot, 0:TAIL]
            else:
                rows_in[at, 2 * LANES : 2 * LANES + 640] = block[192:224, TAIL:]
                rows_in[at, 2 * LANES + 640 :] = block[224:256, TAIL:896]

    @pl.loop(0, steps)
    def _(step):
        for copy in fetch(step):
            copy.wait()
        gate_part = dot(rows_in[...], gate[step])
        up_part = dot(rows_in[...], up[step])
        value = gate_part / (1.0 + jnp.exp(-gate_part)) * up_part
        inner[:, pl.ds(pl.multiple_of(step * 256, 256), 256)] = value.astype(bf16)

    for step in range(steps):
        fetch_down(step).wait()
    for group in range(4):
        mixed[group, 224:256, 896:] = jnp.zeros((32, LANES - 896), bf16)
    for part, (start, width) in enumerate(parts):
        result = dot(inner[...], down[:, start : start + width]).astype(bf16)
        for group in range(4):
            for slot in range(3):
                piece = result[group * 96 + slot * 32 : group * 96 + slot * 32 + 32, :]
                if part < 2:
                    at = 64 * slot + 32 * part
                    mixed[group, at : at + 32, :] = piece
                elif slot < 2:
                    mixed[group, 192 + 32 * slot : 224 + 32 * slot, 0:TAIL] = piece
                else:
                    mixed[group, 192:224, TAIL:] = piece[:, 0:640]
                    mixed[group, 224:256, TAIL:896] = piece[:, 640:]
    for group in range(4):
        send[group * 256 : (group + 1) * 256, :] = dot(scatter, mixed[group]).astype(bf16)


def fill_weights(ids, gates, front, tail_a, tail_b):
    expert = iota((TOK, EXPERTS), 1)
    member = jnp.zeros((TOK, EXPERTS), f32)
    high = jnp.zeros((TOK, EXPERTS), f32)
    low = jnp.zeros((TOK, EXPERTS), f32)
    for k in range(TOP):
        hit = expert == ids[:, k : k + 1]
        value = gates[:, k : k + 1]
        member = member + jnp.where(hit, 1.0, 0.0)
        high = high + jnp.where(hit, (value >> 8).astype(f32), 0.0)
        low = low + jnp.where(hit, (value & 255).astype(f32), 0.0)
    earlier = ones_where(iota((TOK, TOK), 1) < iota((TOK, TOK), 0))
    code = (member * (dot(earlier, member.astype(bf16)) + 1.0)).astype(bf16)
    high = high.astype(bf16)
    low = low.astype(bf16)
    code = jnp.concatenate([code] * 4, axis=0)
    value = jnp.concatenate([high, low, high, low], axis=0)
    spread = ones_where((iota((EXPERTS, SENT), 1) >> 3) == iota((EXPERTS, SENT), 0))
    code = dot(code, spread).astype(jnp.int32)
    value = dot(value, spread)
    row = iota((128, SENT), 1) & 7
    pair = iota((128, SENT), 0) >> 6
    keep = (row < 6) & ((row & 1) == pair) & (code == (row >> 1) + 1)
    front[...] = jnp.where(keep, value, 0.0).astype(bf16)
    keep = (row >= 6) & (pair == 0) & (code == row - 5)
    tail_a[...] = jnp.where(keep, value, 0.0).astype(bf16)
    keep = (row == pair + 6) & (code == 3)
    tail_b[...] = jnp.where(keep, value, 0.0).astype(bf16)


def combine_kernel(recv, tokens, ids, gates, combined, front, tail_a, tail_b):
    fill_weights(ids, gates, front, tail_a, tail_b)

    def join(sums, start):
        return (sums[start : start + 32] * 256.0 + sums[start + 32 : start + 64]) * (
            1.0 / gate_unit
        )

    sums = dot(front[...], recv[...])
    end = 2 * LANES
    combined[:, 0:LANES] = (tokens[:, 0:LANES].astype(f32) + join(sums, 0)).astype(bf16)
    combined[:, LANES:end] = (tokens[:, LANES:end].astype(f32) + join(sums, 64)).astype(bf16)
    first = join(dot(tail_a[...], recv[:, 0:TAIL]), 0)
    second = dot(tail_b[...], recv[:, TAIL:])
    rest = tokens[:, end:].astype(f32)
    combined[:, end : end + 640] = (rest[:, 0:640] + first[:, 0:640] + join(second, 0)).astype(
        bf16
    )
    combined[:, end + 640 :] = (
        rest[:, 640:] + first[:, 640:] + join(second[:, 0:128], 64)
    ).astype(bf16)


def call(kernel, outs, scratch=(), in_specs=None, flops=0, moved=0, limit=None, name=None):
    def whole(_):
        return pl.BlockSpec(memory_space=pltpu.VMEM)

    single = not isinstance(outs, (list, tuple))

    def run(*args):
        return pl.pallas_call(
            kernel,
            out_shape=outs,
            in_specs=in_specs or [whole(a) for a in args],
            out_specs=whole(outs) if single else [whole(o) for o in outs],
            scratch_shapes=list(scratch),
            cost_estimate=pl.CostEstimate(flops=flops, bytes_accessed=moved, transcendentals=0),
            compiler_params=pltpu.CompilerParams(vmem_limit_bytes=limit),
            name=name,
        )(*args)

    return run


def attend_local(queries, latent_cache, cache_lengths):
    requests = queries.shape[0]
    query_block = queries.reshape(requests, HEADS, QK)
    cache_block = latent_cache.reshape(requests, CTX, QK)
    scores = (
        jnp.einsum("rhq,rtq->rht", query_block, cache_block, preferred_element_type=jnp.float32)
        * score_scale
    )
    visible = jnp.arange(CTX, dtype=jnp.int32)[None, None, :] < cache_lengths[:, None, None]
    scores = jnp.where(visible, scores, -jnp.inf)
    peak = jnp.max(scores, axis=2, keepdims=True)
    weights = jnp.exp(scores - peak)
    weights = (weights / jnp.sum(weights, axis=2, keepdims=True)).astype(jnp.bfloat16)
    mixed = jnp.einsum(
        "rht,rtl->rhl", weights, cache_block[:, :, :LATENT], preferred_element_type=jnp.float32
    )
    return mixed.astype(jnp.bfloat16).reshape(requests, HEADS * LATENT)


def exchange(rows):
    blocks = rows.reshape(EXPERTS, ROWS, LANES)
    blocks = lax.all_to_all(blocks, ("wide", "narrow"), split_axis=0, concat_axis=0, tiled=True)
    return blocks.reshape(SENT, LANES)


def on_device(
    tokens,
    norm_gain,
    expert_ids,
    gate_values,
    w_gate,
    w_up,
    w_down,
    queries,
    latent_cache,
    cache_lengths,
):
    sent_shape = jax.ShapeDtypeStruct((SENT, LANES), bf16)
    send = call(
        dispatch_kernel,
        sent_shape,
        scratch=[pltpu.VMEM((128, LANES), bf16)],
        flops=2 * SENT * 128 * LANES,
        moved=4 * 1024 * 1024,
        limit=32 * 1024 * 1024,
        name="dispatch",
    )(tokens, norm_gain.reshape(1, WIDTH), expert_ids.T)
    recv = exchange(send)
    anywhere = pl.BlockSpec(memory_space=pl.ANY)
    worked = call(
        expert_kernel,
        sent_shape,
        scratch=[
            pltpu.VMEM((4, WIDTH, 256), bf16),
            pltpu.VMEM((4, WIDTH, 256), bf16),
            pltpu.VMEM((HID, WIDTH), bf16),
            pltpu.VMEM((384, WIDTH), bf16),
            pltpu.VMEM((384, HID), bf16),
            pltpu.VMEM((4, 256, LANES), bf16),
            pltpu.SemaphoreType.DMA((3, 4)),
        ],
        in_specs=[pl.BlockSpec(memory_space=pltpu.VMEM), anywhere, anywhere, anywhere],
        flops=6 * 384 * WIDTH * HID,
        moved=28 * 1024 * 1024,
        limit=60 * 1024 * 1024,
        name="experts",
    )(recv, w_gate, w_up, w_down)
    returned = exchange(worked)
    combined = call(
        combine_kernel,
        jax.ShapeDtypeStruct((TOK, WIDTH), bf16),
        scratch=[pltpu.VMEM((128, SENT), bf16)] * 3,
        flops=4 * 128 * SENT * LANES,
        moved=4 * 1024 * 1024,
        limit=32 * 1024 * 1024,
        name="combine",
    )(returned, tokens, expert_ids, gate_values)
    attention = attend_local(queries, latent_cache, cache_lengths)
    return (combined, attention)


def solution(mesh):
    both = ("wide", "narrow")
    in_specs = (
        P(both, None),
        P(),
        P(both, None),
        P(both, None),
        P(both, None, None),
        P(both, None, None),
        P(both, None, None),
        P(both, None),
        P(both, None),
        P(both),
    )
    out_specs = (P(both, None), P(both, None))
    return jax.shard_map(
        on_device, mesh=mesh, in_specs=in_specs, out_specs=out_specs, check_vma=False
    )
```
